32 devices in a mesh: qrow: 4 (over y, x), kcol: 8 (over z, core).
Axes of the slice: x: 2, y: 2, z: 4, core: 2. Of those that a mesh axis runs over, the one named last changes fastest.
Arguments:
- queries: bfloat16 [8192, 512], P(('qrow', 'kcol')), may hold values from -6 to 6
- keys: bfloat16 [8192, 128], P(('kcol', 'qrow')), may hold values from -6 to 6
- values: bfloat16 [8192, 128], P(('kcol', 'qrow')), may hold values from -6 to 6
- block_mask: int32 [64, 64], replicated, may hold values from 0 to 1, as said below
Outputs:
- attended: float32 [8192, 512], P(('qrow', 'kcol'))
The draws below stay inside these ranges and needn't reach their ends.
Inputs may be any that keep to these rules, and one draw needn't show every extreme that they name: block_mask[a, b] is 1 only where b <= a, and always where 0 <= a - b < 3.
All inputs are finite; a program needn't handle non-finite values.
Results may differ from the reference program's by a relative error of at most 0.0022.
Values may be sent and summed in bfloat16 or wider, within the bound.
A program may use at most 64 MiB of HBM per device.

```python
import math
import jax
import jax.numpy as jnp
from jax import lax

H = 4
DH = 128
BLOCK = 128
QBT = 16
S = 8192
NB = 64


def draw_queries(key, part):
    base_rows = jnp.clip(jax.random.normal(jax.random.fold_in(key, 11), (S, H * DH)), -6.0, 6.0)
    return base_rows.astype(jnp.bfloat16)


def draw_keys(key, part):
    base_rows = jnp.clip(jax.random.normal(jax.random.fold_in(key, 12), (S, DH)), -6.0, 6.0)
    return base_rows.astype(jnp.bfloat16)


def draw_block_mask(key, part):
    row_ids = jnp.arange(NB, dtype=jnp.int32)[:, None]
    col_ids = jnp.arange(NB, dtype=jnp.int32)[None, :]
    distance = row_ids - col_ids
    picks = jax.random.randint(jax.random.fold_in(key, 14), (NB, NB), 0, 100)
    semantic = (col_ids % 2 == 0) & (picks < 55)
    listed = (distance >= 0) & ((distance < 3) | semantic | (picks < 15))
    return listed.astype(jnp.int32)


def level_of(key, extent, cuts, smallest, top_value):
    gain = 1.0
    for axis_at, blocks in cuts:
        draws = jax.random.uniform(jax.random.fold_in(jax.random.fold_in(key, 6), axis_at), (blocks,), jnp.float32, smallest / len(cuts), top_value / len(cuts))
        gain = gain * jnp.repeat(jnp.exp(draws), extent[axis_at] // blocks).reshape((-1,) + (1,) * (len(extent) - 1 - axis_at))
    return gain


def noise(own_key, shape, scale, most, split=(), kind=jnp.bfloat16):
    level = level_of(own_key, shape, split, -0.22, 0.18) if split else 1.0
    entries = jax.random.normal(own_key, shape, jnp.float32) * scale * level
    return jnp.minimum(jnp.maximum(entries, -most), most).astype(kind)


def setup_inputs(seed: int = 0) -> dict:
    key_list = jax.random.split(jax.random.key(seed), 5)
    return {
        "queries": draw_queries(jax.random.fold_in(key_list[4], 71), 0),
        "keys": draw_keys(jax.random.fold_in(key_list[4], 71), 0),
        "values": noise(key_list[2], (S, DH), 1.0, 6.0, ((0, 32),)),
        "block_mask": draw_block_mask(jax.random.fold_in(key_list[4], 71), 0),
    }


NEG_FILL = -1e+30

def reference(queries, keys, values, block_mask):
    inv_root = 1.0 / math.sqrt(DH)
    query_wide = queries.astype(jnp.float32)
    key_wide = keys.astype(jnp.float32)
    value_wide = values.astype(jnp.float32)
    group_rows = QBT * BLOCK
    pieces = []
    for group in range(S // group_rows):
        end_tok = (group + 1) * group_rows
        end_blk = end_tok // BLOCK
        key_part = key_wide[:end_tok]
        value_part = value_wide[:end_tok].reshape(end_blk, BLOCK, DH)
        key_pos = jnp.arange(end_tok, dtype=jnp.int32)

        def one_block(block_index, key_part=key_part, value_part=value_part, key_pos=key_pos, end_blk=end_blk):
            first_row = block_index * BLOCK
            query_heads = lax.dynamic_slice_in_dim(query_wide, first_row, BLOCK, 0).reshape(BLOCK, H, DH)
            scores = jnp.einsum('rhd,kd->hrk', query_heads, key_part, precision=lax.Precision.HIGHEST) * inv_root
            mask_row = lax.dynamic_index_in_dim(block_mask, block_index, 0, keepdims=False)[:end_blk]
            listed = jnp.repeat(mask_row, BLOCK) == 1
            query_pos = first_row + jnp.arange(BLOCK, dtype=jnp.int32)
            permitted = listed[None, :] & (key_pos[None, :] <= query_pos[:, None])
            permitted = permitted.reshape(BLOCK, end_blk, BLOCK)
            scores = scores.reshape(H, BLOCK, end_blk, BLOCK)
            scores = jnp.where(permitted[None], scores, NEG_FILL)
            block_top = lax.optimization_barrier(jnp.max(scores, axis=3))
            weights = jnp.where(permitted[None], jnp.exp(scores - block_top[..., None]), 0.0).astype(jnp.bfloat16)
            weights_wide = weights.astype(jnp.float32)
            block_mass = lax.optimization_barrier(jnp.sum(weights_wide, axis=3))
            block_out = jnp.einsum('hrkb,kbd->hrkd', weights_wide, value_part, precision=lax.Precision.HIGHEST)
            row_top = lax.optimization_barrier(jnp.max(block_top, axis=2))
            factor = jnp.exp(block_top - row_top[..., None])
            numerator = lax.optimization_barrier(jnp.sum(block_out * factor[..., None], axis=2))
            denominator = lax.optimization_barrier(jnp.sum(block_mass * factor, axis=2))
            mixed = numerator / denominator[..., None]
            return jnp.transpose(mixed, (1, 0, 2)).reshape(BLOCK, H * DH)
        first_blk = group * group_rows // BLOCK
        outs_group = lax.map(one_block, jnp.arange(first_blk, end_blk, dtype=jnp.int32))
        pieces.append(outs_group.reshape(group_rows, H * DH))
    return jnp.concatenate(pieces, axis=0)
```

```python
import math

import jax
import jax.numpy as jnp
from jax import lax
from jax.experimental import pallas as pl
from jax.experimental.pallas import tpu as pltpu
from jax.sharding import PartitionSpec as P

H = 4
DH = 128
BLOCK = 128
GROUP = 4
NEG_FILL = -1e30
SCALE = math.log2(math.e) / math.sqrt(DH)


def over_keys(values, weights):
    return lax.dot_general(
        values, weights, (((0,), (0,)), ((), ())), preferred_element_type=jnp.float32
    )


def attend(mask_ref, q_ref, k_ref, v_ref, out_ref, listed, total):
    own_blocks = q_ref.shape[0] // BLOCK
    device = lax.axis_index("qrow") * lax.axis_size("kcol") + lax.axis_index("kcol")

    def rows_of(ref, block):
        return ref[pl.ds(pl.multiple_of(block * BLOCK, BLOCK), BLOCK), :]

    for own in range(own_blocks):
        rows = pl.ds(own * BLOCK, BLOCK)
        row = device * own_blocks + own
        flipped = jnp.concatenate(
            [q_ref[rows, h * DH : (h + 1) * DH].T for h in range(H)], axis=1
        )

        def note(j, count):
            listed[count] = j
            return count + mask_ref[row, j]

        count = lax.fori_loop(0, row, note, jnp.int32(0))

        def scores_of(block):
            return jnp.dot(rows_of(k_ref, block), flipped, preferred_element_type=jnp.float32)

        scores = scores_of(row)
        key_at = lax.broadcasted_iota(jnp.int32, scores.shape, 0)
        query_at = lax.broadcasted_iota(jnp.int32, scores.shape, 1) % BLOCK
        scores = jnp.where(key_at <= query_at, scores, NEG_FILL)
        top = jnp.max(scores, axis=0, keepdims=True)
        weights = jnp.exp2(scores * SCALE - top * SCALE)
        mass = jnp.sum(weights, axis=0, keepdims=True)
        total[...] = over_keys(rows_of(v_ref, row), weights.astype(jnp.bfloat16))

        def add(start, size, state):
            top, mass = state
            blocks = [listed[start + g] for g in range(size)]
            scores = [scores_of(b) for b in blocks]
            high = scores[0]
            for s in scores[1:]:
                high = jnp.maximum(high, s)
            new_top = jnp.maximum(top, jnp.max(high, axis=0, keepdims=True))
            fade = jnp.exp2((top - new_top) * SCALE)
            shift = new_top * SCALE
            weights = [jnp.exp2(s * SCALE - shift) for s in scores]
            summed = weights[0]
            for w in weights[1:]:
                summed = summed + w
            mass = mass * fade + jnp.sum(summed, axis=0, keepdims=True)
            part = over_keys(
                jnp.concatenate([rows_of(v_ref, b) for b in blocks], axis=0),
                jnp.concatenate([w.astype(jnp.bfloat16) for w in weights], axis=0),
            )
            total[...] = total[...] * fade + part
            return new_top, mass

        groups = count // GROUP
        state = lax.fori_loop(0, groups, lambda t, c: add(t * GROUP, GROUP, c), (top, mass))
        top, mass = lax.fori_loop(groups * GROUP, count, lambda t, c: add(t, 1, c), state)
        result = total[...] / mass
        for h in range(H):
            out_ref[rows, h * DH : (h + 1) * DH] = result[:, h * BLOCK : (h + 1) * BLOCK].T


def shards(queries, keys, values, block_mask):
    all_keys = lax.all_gather(keys, ("kcol", "qrow"), axis=0, tiled=True)
    all_values = lax.all_gather(values, ("kcol", "qrow"), axis=0, tiled=True)
    vmem = pl.BlockSpec(memory_space=pltpu.VMEM)
    return pl.pallas_call(
        attend,
        out_shape=jax.ShapeDtypeStruct(queries.shape, jnp.float32),
        in_specs=[pl.BlockSpec(memory_space=pltpu.SMEM), vmem, vmem, vmem],
        out_specs=vmem,
        scratch_shapes=[
            pltpu.SMEM((block_mask.shape[1],), jnp.int32),
            pltpu.VMEM((DH, H * BLOCK), jnp.float32),
        ],
        compiler_params=pltpu.CompilerParams(vmem_limit_bytes=48 * 2**20),
    )(block_mask, queries, all_keys, all_values)


def solution(mesh):
    placed = (P(("qrow", "kcol"), None), P(("kcol", "qrow"), None), P(("kcol", "qrow"), None), P())
    return jax.shard_map(
        shards, mesh=mesh, in_specs=placed, out_specs=P(("qrow", "kcol"), None), check_vma=False
    )
```

```python
import math

import jax
import jax.numpy as jnp
from jax import lax
from jax.experimental import pallas as pl
from jax.experimental.pallas import tpu as pltpu
from jax.sharding import PartitionSpec as P

H = 4
DH = 128
BLOCK = 128
GROUP = 4
MOST = 64
NEG_FILL = -1e30
SCALE = math.log2(math.e) / math.sqrt(DH)


def over_keys(values, weights):
    return lax.dot_general(
        values, weights, (((0,), (0,)), ((), ())), preferred_element_type=jnp.float32
    )


def attend(mask_ref, q_ref, k_ref, v_ref, out_ref, listed, total):
    own_blocks = q_ref.shape[0] // BLOCK
    device = lax.axis_index("qrow") * lax.axis_size("kcol") + lax.axis_index("kcol")

    def rows_of(ref, block):
        return ref[pl.ds(pl.multiple_of(block * BLOCK, BLOCK), BLOCK), :]

    for own in range(own_blocks):
        rows = pl.ds(own * BLOCK, BLOCK)
        row = device * own_blocks + own
        flipped = jnp.concatenate(
            [q_ref[rows, h * DH : (h + 1) * DH].T for h in range(H)], axis=1
        )

        def note(j, count):
            listed[count] = j
            return count + mask_ref[row, j]

        count = lax.fori_loop(0, row, note, jnp.int32(0))

        def scores_of(block):
            return jnp.dot(rows_of(k_ref, block), flipped, preferred_element_type=jnp.float32)

        scores = scores_of(row)
        key_at = lax.broadcasted_iota(jnp.int32, scores.shape, 0)
        query_at = lax.broadcasted_iota(jnp.int32, scores.shape, 1) % BLOCK
        scores = jnp.where(key_at <= query_at, scores, NEG_FILL)
        top = jnp.max(scores, axis=0, keepdims=True)
        weights = jnp.exp2(scores * SCALE - top * SCALE)
        mass = jnp.sum(weights, axis=0, keepdims=True)
        total[...] = over_keys(rows_of(v_ref, row), weights.astype(jnp.bfloat16))

        def add(start, size, state):
            top, mass = state
            blocks = [listed[start + g] for g in range(size)]
            scores = [scores_of(b) for b in blocks]
            high = scores[0]
            for s in scores[1:]:
                high = jnp.maximum(high, s)
            new_top = jnp.maximum(top, jnp.max(high, axis=0, keepdims=True))
            fade = jnp.exp2((top - new_top) * SCALE)
            shift = new_top * SCALE
            weights = [jnp.exp2(s * SCALE - shift) for s in scores]
            summed = weights[0]
            for w in weights[1:]:
                summed = summed + w
            mass = mass * fade + jnp.sum(summed, axis=0, keepdims=True)
            part = over_keys(
                jnp.concatenate([rows_of(v_ref, b) for b in blocks], axis=0),
                jnp.concatenate([w.astype(jnp.bfloat16) for w in weights], axis=0),
            )
            total[...] = total[...] * fade + part
            return new_top, mass

        groups = count // GROUP
        state = lax.fori_loop(0, groups, lambda t, c: add(t * GROUP, GROUP, c), (top, mass))
        top, mass = lax.fori_loop(groups * GROUP, count, lambda t, c: add(t, 1, c), state)
        result = total[...] / mass
        for h in range(H):
            out_ref[rows, h * DH : (h + 1) * DH] = result[:, h * BLOCK : (h + 1) * BLOCK].T


def spread(k_ref, v_ref, k_all, v_all, send, recv, local):
    ring, lane = lax.axis_size("kcol"), lax.axis_size("qrow")
    depth, width = ring // 2, lane // 2
    q, c = lax.axis_index("qrow"), lax.axis_index("kcol")
    level, core = c // 2, c % 2
    high, low = q // width, q % width
    tokens = k_ref.shape[0]
    own, whole = (k_ref, v_ref), (k_all, v_all)
    sibling = {"qrow": q, "kcol": level * 2 + (1 - core)}
    over = {"qrow": (1 - high) * width + low, "kcol": c}
    sides = [(low + i) % width for i in range(1, width)]
    beside = [{"qrow": high * width + i, "kcol": c} for i in sides]
    up = {"qrow": q, "kcol": c + 2}
    down = {"qrow": q, "kcol": c - 2}
    has_up, has_down = level < depth - 1, level > 0

    def slot(at, column, parity=core):
        return (at * 2 + parity) * lane + column

    def place(kv, block):
        return whole[kv].at[pl.ds(pl.multiple_of(block * tokens, tokens), tokens), :]

    barrier = pltpu.get_barrier_semaphore()

    def greet(target):
        pl.semaphore_signal(
            barrier, inc=1, device_id=target, device_id_type=pl.DeviceIdType.MESH
        )

    for target in [sibling, over] + beside:
        greet(target)
    pl.when(has_up)(lambda: greet(up))
    pl.when(has_down)(lambda: greet(down))
    ends = has_up.astype(jnp.int32) + has_down.astype(jnp.int32)
    pl.semaphore_wait(barrier, 2 + len(beside) + ends)

    started = []

    def landed(ok, kv, block):
        @pl.when(ok)
        def _():
            here = place(kv, block)
            pltpu.make_async_copy(here, here, recv.at[kv, block]).wait()

    def push(ok, kv, block, target, kind, at, source=None):
        copy = pltpu.make_async_remote_copy(
            src_ref=place(kv, block) if source is None else source,
            dst_ref=place(kv, block),
            send_sem=send.at[kind, at],
            recv_sem=recv.at[kv, block],
            device_id=target,
            device_id_type=pl.DeviceIdType.MESH,
        )
        pl.when(ok)(copy.start)
        started.append((ok, copy))

    def column_sends(ok, at, way):
        block = slot(at, q)
        for kv in range(2):
            source = own[kv] if way == 0 else None
            if way == 0:
                push(has_up, kv, block, up, 0 + kv, at, source)
                push(has_down, kv, block, down, 2 + kv, at, source)
            else:
                landed(ok, kv, block)
                if way > 0:
                    push(ok & has_up, kv, block, up, 0 + kv, at)
                else:
                    push(ok & has_down, kv, block, down, 2 + kv, at)
            push(ok, kv, block, over, 4 + kv, at, source)
            for i, target in enumerate(beside):
                push(ok, kv, block, target, 8 + 2 * i + kv, at, source)
            push(ok, kv, block, sibling, 6 + kv, at, source)

    base = 8 + 2 * len(beside)

    def relays(ok, at):
        kind = base
        for i in sides:
            block = slot(at, high * width + i)
            landed(ok, 0, block)
            push(ok, 0, block, over, kind, at)
            push(ok, 0, block, sibling, kind + 1, at)
            kind += 2
        block = slot(at, (1 - high) * width + low)
        for kv in (1, 0):
            landed(ok, kv, block)
            if kv == 1:
                for target in beside:
                    push(ok, 1, block, target, kind, at)
                    kind += 1
            push(ok, kv, block, sibling, kind, at)
            kind += 1
        for i in sides:
            block = slot(at, high * width + i)
            landed(ok, 1, block)
            push(ok, 1, block, sibling, kind, at)
            kind += 1

    last = base + 4 * len(beside) + 2

    def corners(ok, at):
        kind = last
        for i in sides:
            block = slot(at, (1 - high) * width + i)
            for kv in range(2):
                landed(ok, kv, block)
                push(ok, kv, block, sibling, kind, at)
                kind += 1

    def positions(step):
        if step == 0:
            return [(level >= 0, level, 0)]
        return [
            (level >= step, level - step, 1),
            (level + step < depth, level + step, -1),
        ]

    copies = []
    for step in range(depth + 2):
        if step < depth:
            for ok, at, way in positions(step):
                column_sends(ok, at, way)
        if step == 0:
            for kv in range(2):
                copy = pltpu.make_async_copy(own[kv], place(kv, slot(level, q)), local.at[kv])
                copy.start()
                copies.append(copy)
        if 1 <= step <= depth:
            for ok, at, _ in positions(step - 1):
                relays(ok, at)
        if step >= 2:
            for ok, at, _ in positions(step - 2):
                corners(ok, at)
    for copy in copies:
        copy.wait()
    for at in range(depth):
        for column in range(lane):
            for kv in range(2):
                landed(level >= 0, kv, slot(at, column, 1 - core))
    for ok, copy in started:
        pl.when(ok)(copy.wait_send)


def gathered(keys, values):
    ring, lane = lax.axis_size("kcol"), lax.axis_size("qrow")
    devices = ring * lane
    if ring % 2 or lane % 2 or devices > MOST:
        both = ("kcol", "qrow")
        return (
            lax.all_gather(keys, both, axis=0, tiled=True),
            lax.all_gather(values, both, axis=0, tiled=True),
        )
    vmem = pl.BlockSpec(memory_space=pltpu.VMEM)
    full = jax.ShapeDtypeStruct((keys.shape[0] * devices, keys.shape[1]), keys.dtype)
    side = lane // 2 - 1
    return pl.pallas_call(
        spread,
        out_shape=(full, full),
        in_specs=[vmem, vmem],
        out_specs=(vmem, vmem),
        scratch_shapes=[
            pltpu.SemaphoreType.DMA((10 + 8 * side, ring // 2)),
            pltpu.SemaphoreType.DMA((2, devices)),
            pltpu.SemaphoreType.DMA((2,)),
        ],
        compiler_params=pltpu.CompilerParams(
            collective_id=0, has_side_effects=True, vmem_limit_bytes=32 * 2**20
        ),
    )(keys, values)


def shards(queries, keys, values, block_mask):
    all_keys, all_values = gathered(keys, values)
    vmem = pl.BlockSpec(memory_space=pltpu.VMEM)
    return pl.pallas_call(
        attend,
        out_shape=jax.ShapeDtypeStruct(queries.shape, jnp.float32),
        in_specs=[pl.BlockSpec(memory_space=pltpu.SMEM), vmem, vmem, vmem],
        out_specs=vmem,
        scratch_shapes=[
            pltpu.SMEM((block_mask.shape[1],), jnp.int32),
            pltpu.VMEM((DH, H * BLOCK), jnp.float32),
        ],
        compiler_params=pltpu.CompilerParams(vmem_limit_bytes=48 * 2**20),
    )(block_mask, queries, all_keys, all_values)


def solution(mesh):
    placed = (P(("qrow", "kcol"), None), P(("kcol", "qrow"), None), P(("kcol", "qrow"), None), P())
    return jax.shard_map(
        shards, mesh=mesh, in_specs=placed, out_specs=P(("qrow", "kcol"), None), check_vma=False
    )
```

```python
import math

import jax
import jax.numpy as jnp
from jax import lax
from jax.experimental import pallas as pl
from jax.experimental.pallas import tpu as pltpu
from jax.sharding import PartitionSpec as P

H = 4
DH = 128
BLOCK = 128
GROUPS = (8, 4, 2, 1)
MOST = 64
NEG_FILL = -1e30
SCALE = math.log2(math.e) / math.sqrt(DH)


def over_keys(values, weights):
    return lax.dot_general(
        values, weights, (((0,), (0,)), ((), ())), preferred_element_type=jnp.float32
    )


def attend(mask_ref, q_ref, k_ref, v_ref, out_ref, listed, total, held, sent):
    own_blocks = q_ref.shape[0] // BLOCK
    device = lax.axis_index("qrow") * lax.axis_size("kcol") + lax.axis_index("kcol")

    def rows_of(ref, block):
        return ref[pl.ds(pl.multiple_of(block * BLOCK, BLOCK), BLOCK), :]

    copies = []
    for own in range(own_blocks):
        rows = pl.ds(own * BLOCK, BLOCK)
        row = device * own_blocks + own
        flipped = jnp.concatenate(
            [q_ref[rows, h * DH : (h + 1) * DH].T for h in range(H)], axis=1
        )

        def note(j, count):
            listed[count] = j
            return count + mask_ref[row, j]

        count = lax.fori_loop(0, row, note, jnp.int32(0))

        def scores_of(block):
            return jnp.dot(rows_of(k_ref, block), flipped, preferred_element_type=jnp.float32)

        scores = scores_of(row)
        key_at = lax.broadcasted_iota(jnp.int32, scores.shape, 0)
        query_at = lax.broadcasted_iota(jnp.int32, scores.shape, 1) % BLOCK
        scores = jnp.where(key_at <= query_at, scores, NEG_FILL)
        top = jnp.max(scores, axis=0, keepdims=True)
        weights = jnp.exp2(scores * SCALE - top * SCALE)
        mass = jnp.sum(weights, axis=0, keepdims=True)
        total[...] = over_keys(rows_of(v_ref, row), weights.astype(jnp.bfloat16))

        def add(start, size, state):
            top, mass = state
            blocks = [listed[start + g] for g in range(size)]
            scores = [scores_of(b) for b in blocks]
            high = scores[0]
            for s in scores[1:]:
                high = jnp.maximum(high, s)
            new_top = jnp.maximum(top, jnp.max(high, axis=0, keepdims=True))
            fade = jnp.exp2((top - new_top) * SCALE)
            shift = new_top * SCALE
            weights = [jnp.exp2(s * SCALE - shift) for s in scores]
            summed = weights[0]
            for w in weights[1:]:
                summed = summed + w
            mass = mass * fade + jnp.sum(summed, axis=0, keepdims=True)
            part = over_keys(
                jnp.concatenate([rows_of(v_ref, b) for b in blocks], axis=0),
                jnp.concatenate([w.astype(jnp.bfloat16) for w in weights], axis=0),
            )
            total[...] = total[...] * fade + part
            return new_top, mass

        state, done = (top, mass), jnp.int32(0)
        for size in GROUPS:
            trips = (count - done) // size
            state = lax.fori_loop(
                0, trips, lambda t, c: add(done + t * size, size, c), state
            )
            done = done + trips * size
        mass = state[1]
        result = total[...] / mass
        for h in range(H):
            held[rows, h * DH : (h + 1) * DH] = result[:, h * BLOCK : (h + 1) * BLOCK].T
        copy = pltpu.make_async_copy(held.at[rows, :], out_ref.at[rows, :], sent.at[own])
        copy.start()
        copies.append(copy)
    for copy in copies:
        copy.wait()


def spread(k_ref, v_ref, k_all, v_all, send, recv, local):
    ring, lane = lax.axis_size("kcol"), lax.axis_size("qrow")
    depth, width = ring // 2, lane // 2
    q, c = lax.axis_index("qrow"), lax.axis_index("kcol")
    level, core = c // 2, c % 2
    high, low = q // width, q % width
    tokens = k_ref.shape[0]
    own, whole = (k_ref, v_ref), (k_all, v_all)
    sibling = {"qrow": q, "kcol": level * 2 + (1 - core)}
    over = {"qrow": (1 - high) * width + low, "kcol": c}
    sides = [(low + i) % width for i in range(1, width)]
    beside = [{"qrow": high * width + i, "kcol": c} for i in sides]
    up = {"qrow": q, "kcol": c + 2}
    down = {"qrow": q, "kcol": c - 2}
    has_up, has_down = level < depth - 1, level > 0

    def slot(at, column, parity=core):
        return (at * 2 + parity) * lane + column

    def place(kv, block):
        return whole[kv].at[pl.ds(pl.multiple_of(block * tokens, tokens), tokens), :]

    copies = [
        pltpu.make_async_copy(own[kv], place(kv, slot(level, q)), local.at[kv]) for kv in range(2)
    ]
    for copy in copies:
        copy.start()

    barrier = pltpu.get_barrier_semaphore()

    def greet(target):
        pl.semaphore_signal(
            barrier, inc=1, device_id=target, device_id_type=pl.DeviceIdType.MESH
        )

    for target in [sibling, over] + beside:
        greet(target)
    pl.when(has_up)(lambda: greet(up))
    pl.when(has_down)(lambda: greet(down))
    ends = has_up.astype(jnp.int32) + has_down.astype(jnp.int32)
    pl.semaphore_wait(barrier, 2 + len(beside) + ends)

    for copy in copies:
        copy.wait()
    started = []

    def landed(ok, kv, block):
        @pl.when(ok)
        def _():
            here = place(kv, block)
            pltpu.make_async_copy(here, here, recv.at[kv, block]).wait()

    def push(ok, kv, block, target, kind, at):
        copy = pltpu.make_async_remote_copy(
            src_ref=place(kv, block),
            dst_ref=place(kv, block),
            send_sem=send.at[kind, at],
            recv_sem=recv.at[kv, block],
            device_id=target,
            device_id_type=pl.DeviceIdType.MESH,
        )
        pl.when(ok)(copy.start)
        started.append((ok, copy))

    def column_sends(ok, at, way):
        block = slot(at, q)
        for kv in range(2):
            if way == 0:
                push(has_up, kv, block, up, 0 + kv, at)
                push(has_down, kv, block, down, 2 + kv, at)
            else:
                landed(ok, kv, block)
                if way > 0:
                    push(ok & has_up, kv, block, up, 0 + kv, at)
                else:
                    push(ok & has_down, kv, block, down, 2 + kv, at)
            push(ok, kv, block, over, 4 + kv, at)
            for i, target in enumerate(beside):
                push(ok, kv, block, target, 8 + 2 * i + kv, at)
            push(ok, kv, block, sibling, 6 + kv, at)

    base = 8 + 2 * len(beside)

    def relays(ok, at):
        kind = base
        for i in sides:
            block = slot(at, high * width + i)
            landed(ok, 0, block)
            push(ok, 0, block, over, kind, at)
            push(ok, 0, block, sibling, kind + 1, at)
            kind += 2
        block = slot(at, (1 - high) * width + low)
        for kv in (1, 0):
            landed(ok, kv, block)
            if kv == 1:
                for target in beside:
                    push(ok, 1, block, target, kind, at)
                    kind += 1
            push(ok, kv, block, sibling, kind, at)
            kind += 1
        for i in sides:
            block = slot(at, high * width + i)
            landed(ok, 1, block)
            push(ok, 1, block, sibling, kind, at)
            kind += 1

    last = base + 4 * len(beside) + 2

    def corners(ok, at):
        kind = last
        for i in sides:
            block = slot(at, (1 - high) * width + i)
            for kv in range(2):
                landed(ok, kv, block)
                push(ok, kv, block, sibling, kind, at)
                kind += 1

    def positions(step):
        if step == 0:
            return [(level >= 0, level, 0)]
        return [
            (level >= step, level - step, 1),
            (level + step < depth, level + step, -1),
        ]

    for step in range(depth + 2):
        if step < depth:
            for ok, at, way in positions(step):
                column_sends(ok, at, way)
        if 1 <= step <= depth:
            for ok, at, _ in positions(step - 1):
                relays(ok, at)
        if step >= 2:
            for ok, at, _ in positions(step - 2):
                corners(ok, at)
    for at in range(depth):
        for column in range(lane):
            for kv in range(2):
                landed(level >= 0, kv, slot(at, column, 1 - core))
    for ok, copy in started:
        pl.when(ok)(copy.wait_send)


def gathered(keys, values):
    ring, lane = lax.axis_size("kcol"), lax.axis_size("qrow")
    devices = ring * lane
    if ring % 2 or lane % 2 or devices > MOST:
        both = ("kcol", "qrow")
        return (
            lax.all_gather(keys, both, axis=0, tiled=True),
            lax.all_gather(values, both, axis=0, tiled=True),
        )
    vmem = pl.BlockSpec(memory_space=pltpu.VMEM)
    full = jax.ShapeDtypeStruct((keys.shape[0] * devices, keys.shape[1]), keys.dtype)
    side = lane // 2 - 1
    return pl.pallas_call(
        spread,
        out_shape=(full, full),
        in_specs=[pl.BlockSpec(memory_space=pltpu.HBM)] * 2,
        out_specs=(vmem, vmem),
        scratch_shapes=[
            pltpu.SemaphoreType.DMA((10 + 8 * side, ring // 2)),
            pltpu.SemaphoreType.DMA((2, devices)),
            pltpu.SemaphoreType.DMA((2,)),
        ],
        compiler_params=pltpu.CompilerParams(
            collective_id=0, has_side_effects=True, vmem_limit_bytes=32 * 2**20
        ),
    )(keys, values)


def shards(queries, keys, values, block_mask):
    all_keys, all_values = gathered(keys, values)
    vmem = pl.BlockSpec(memory_space=pltpu.VMEM)
    return pl.pallas_call(
        attend,
        out_shape=jax.ShapeDtypeStruct(queries.shape, jnp.float32),
        in_specs=[pl.BlockSpec(memory_space=pltpu.SMEM), vmem, vmem, vmem],
        out_specs=pl.BlockSpec(memory_space=pltpu.HBM),
        scratch_shapes=[
            pltpu.SMEM((block_mask.shape[1],), jnp.int32),
            pltpu.VMEM((DH, H * BLOCK), jnp.float32),
            pltpu.VMEM(queries.shape, jnp.float32),
            pltpu.SemaphoreType.DMA((queries.shape[0] // BLOCK,)),
        ],
        compiler_params=pltpu.CompilerParams(vmem_limit_bytes=48 * 2**20),
    )(block_mask, queries, all_keys, all_values)


def solution(mesh):
    placed = (P(("qrow", "kcol"), None), P(("kcol", "qrow"), None), P(("kcol", "qrow"), None), P())
    return jax.shard_map(
        shards, mesh=mesh, in_specs=placed, out_specs=P(("qrow", "kcol"), None), check_vma=False
    )
```

```python
import math

import jax
import jax.numpy as jnp
from jax import lax
from jax.experimental import pallas as pl
from jax.experimental.pallas import tpu as pltpu
from jax.sharding import PartitionSpec as P

H = 4
DH = 128
BLOCK = 128
GROUPS = (8, 4, 2, 1)
MOST = 64
NEG_FILL = -1e30
SCALE = math.log2(math.e) / math.sqrt(DH)


def over_keys(values, weights):
    return lax.dot_general(
        values, weights, (((0,), (0,)), ((), ())), preferred_element_type=jnp.float32
    )


def attend(mask_ref, q_ref, k_ref, v_ref, out_ref, listed, total, held, sent):
    own_blocks = q_ref.shape[0] // BLOCK
    device = lax.axis_index("qrow") * lax.axis_size("kcol") + lax.axis_index("kcol")

    def rows_of(ref, block):
        return ref[pl.ds(pl.multiple_of(block * BLOCK, BLOCK), BLOCK), :]

    copies = []
    for own in range(own_blocks):
        rows = pl.ds(own * BLOCK, BLOCK)
        row = device * own_blocks + own
        flipped = jnp.concatenate(
            [q_ref[rows, h * DH : (h + 1) * DH].T for h in range(H)], axis=1
        )

        def note(j, count):
            listed[count] = j
            return count + mask_ref[row, j]

        count = lax.fori_loop(0, row, note, jnp.int32(0))

        def scores_of(block):
            return jnp.dot(rows_of(k_ref, block), flipped, preferred_element_type=jnp.float32)

        scores = scores_of(row)
        key_at = lax.broadcasted_iota(jnp.int32, scores.shape, 0)
        query_at = lax.broadcasted_iota(jnp.int32, scores.shape, 1) % BLOCK
        scores = jnp.where(key_at <= query_at, scores, NEG_FILL)
        top = jnp.max(scores, axis=0, keepdims=True)
        weights = jnp.exp2(scores * SCALE - top * SCALE)
        mass = jnp.sum(weights, axis=0, keepdims=True)
        total[...] = over_keys(rows_of(v_ref, row), weights.astype(jnp.bfloat16))

        def add(start, size, state):
            top, mass = state
            blocks = [listed[start + g] for g in range(size)]
            scores = [scores_of(b) for b in blocks]
            high = scores[0]
            for s in scores[1:]:
                high = jnp.maximum(high, s)
            new_top = jnp.maximum(top, jnp.max(high, axis=0, keepdims=True))
            fade = jnp.exp2((top - new_top) * SCALE)
            shift = new_top * SCALE
            weights = [jnp.exp2(s * SCALE - shift) for s in scores]
            summed = weights[0]
            for w in weights[1:]:
                summed = summed + w
            mass = mass * fade + jnp.sum(summed, axis=0, keepdims=True)
            part = over_keys(
                jnp.concatenate([rows_of(v_ref, b) for b in blocks], axis=0),
                jnp.concatenate([w.astype(jnp.bfloat16) for w in weights], axis=0),
            )
            total[...] = total[...] * fade + part
            return new_top, mass

        state, done = (top, mass), jnp.int32(0)
        for size in GROUPS:
            trips = (count - done) // size
            state = lax.fori_loop(
                0, trips, lambda t, c: add(done + t * size, size, c), state
            )
            done = done + trips * size
        mass = state[1]
        result = total[...] / mass
        for h in range(H):
            held[rows, h * DH : (h + 1) * DH] = result[:, h * BLOCK : (h + 1) * BLOCK].T
        copy = pltpu.make_async_copy(held.at[rows, :], out_ref.at[rows, :], sent.at[own])
        copy.start()
        copies.append(copy)
    for copy in copies:
        copy.wait()


def spread(k_ref, v_ref, k_all, v_all, send, recv, local):
    ring, lane = lax.axis_size("kcol"), lax.axis_size("qrow")
    depth, width = ring // 2, lane // 2
    q, c = lax.axis_index("qrow"), lax.axis_index("kcol")
    level, core = c // 2, c % 2
    high, low = q // width, q % width
    tokens = k_ref.shape[0]
    own, whole = (k_ref, v_ref), (k_all, v_all)
    sibling = {"qrow": q, "kcol": level * 2 + (1 - core)}
    over = {"qrow": (1 - high) * width + low, "kcol": c}
    sides = [(low + i) % width for i in range(1, width)]
    beside = [{"qrow": high * width + i, "kcol": c} for i in sides]
    up = {"qrow": q, "kcol": c + 2}
    down = {"qrow": q, "kcol": c - 2}
    has_up, has_down = level < depth - 1, level > 0

    def slot(at, column, parity=core):
        return (at * 2 + parity) * lane + column

    def place(kv, block):
        return whole[kv].at[pl.ds(pl.multiple_of(block * tokens, tokens), tokens), :]

    copies = [
        pltpu.make_async_copy(own[kv], place(kv, slot(level, q)), local.at[kv]) for kv in range(2)
    ]
    for copy in copies:
        copy.start()

    barrier = pltpu.get_barrier_semaphore()

    def greet(target):
        pl.semaphore_signal(
            barrier, inc=1, device_id=target, device_id_type=pl.DeviceIdType.MESH
        )

    for target in [sibling, over] + beside:
        greet(target)
    pl.when(has_up)(lambda: greet(up))
    pl.when(has_down)(lambda: greet(down))
    ends = has_up.astype(jnp.int32) + has_down.astype(jnp.int32)
    pl.semaphore_wait(barrier, 2 + len(beside) + ends)

    for copy in copies:
        copy.wait()
    started = []

    def landed(ok, kv, block):
        @pl.when(ok)
        def _():
            here = place(kv, block)
            pltpu.make_async_copy(here, here, recv.at[kv, block]).wait()

    def push(ok, kv, block, target, kind, at):
        copy = pltpu.make_async_remote_copy(
            src_ref=place(kv, block),
            dst_ref=place(kv, block),
            send_sem=send.at[kind, at],
            recv_sem=recv.at[kv, block],
            device_id=target,
            device_id_type=pl.DeviceIdType.MESH,
        )
        pl.when(ok)(copy.start)
        started.append((ok, copy))

    def column_sends(ok, at, way):
        block = slot(at, q)
        for kv in range(2):
            if way == 0:
                push(has_up, kv, block, up, 0 + kv, at)
                push(has_down, kv, block, down, 2 + kv, at)
            else:
                landed(ok, kv, block)
                if way > 0:
                    push(ok & has_up, kv, block, up, 0 + kv, at)
                else:
                    push(ok & has_down, kv, block, down, 2 + kv, at)
            push(ok, kv, block, over, 4 + kv, at)
            for i, target in enumerate(beside):
                push(ok, kv, block, target, 8 + 2 * i + kv, at)
            push(ok, kv, block, sibling, 6 + kv, at)

    base = 8 + 2 * len(beside)

    def relays(ok, at):
        kind = base
        for i in sides:
            block = slot(at, high * width + i)
            landed(ok, 0, block)
            push(ok, 0, block, over, kind, at)
            push(ok, 0, block, sibling, kind + 1, at)
            kind += 2
        block = slot(at, (1 - high) * width + low)
        for kv in (1, 0):
            landed(ok, kv, block)
            if kv == 1:
                for target in beside:
                    push(ok, 1, block, target, kind, at)
                    kind += 1
            push(ok, kv, block, sibling, kind, at)
            kind += 1
        for i in sides:
            block = slot(at, high * width + i)
            landed(ok, 1, block)
            push(ok, 1, block, sibling, kind, at)
            kind += 1

    last = base + 4 * len(beside) + 2

    def corners(ok, at):
        kind = last
        for i in sides:
            block = slot(at, (1 - high) * width + i)
            for kv in range(2):
                landed(ok, kv, block)
                push(ok, kv, block, sibling, kind, at)
                kind += 1

    def positions(step):
        if step == 0:
            return [(level >= 0, level, 0)]
        return [
            (level >= step, level - step, 1),
            (level + step < depth, level + step, -1),
        ]

    for step in range(depth + 2):
        if step < depth:
            for ok, at, way in positions(step):
                column_sends(ok, at, way)
        if 1 <= step <= depth:
            for ok, at, _ in positions(step - 1):
                relays(ok, at)
        if step >= 2:
            for ok, at, _ in positions(step - 2):
                corners(ok, at)
    for at in range(depth):
        for column in range(lane):
            for kv in range(2):
                landed(level >= 0, kv, slot(at, column, 1 - core))
    for ok, copy in started:
        pl.when(ok)(copy.wait_send)


def in_hbm(array):
    return pltpu.with_memory_space_constraint(array, pltpu.HBM)


def gathered(keys, values):
    ring, lane = lax.axis_size("kcol"), lax.axis_size("qrow")
    devices = ring * lane
    if ring % 2 or lane % 2 or devices > MOST:
        both = ("kcol", "qrow")
        return (
            lax.all_gather(keys, both, axis=0, tiled=True),
            lax.all_gather(values, both, axis=0, tiled=True),
        )
    vmem = pl.BlockSpec(memory_space=pltpu.VMEM)
    full = jax.ShapeDtypeStruct((keys.shape[0] * devices, keys.shape[1]), keys.dtype)
    side = lane // 2 - 1
    return pl.pallas_call(
        spread,
        out_shape=(full, full),
        in_specs=[pl.BlockSpec(memory_space=pltpu.HBM)] * 2,
        out_specs=(vmem, vmem),
        scratch_shapes=[
            pltpu.SemaphoreType.DMA((10 + 8 * side, ring // 2)),
            pltpu.SemaphoreType.DMA((2, devices)),
            pltpu.SemaphoreType.DMA((2,)),
        ],
        compiler_params=pltpu.CompilerParams(
            collective_id=0, has_side_effects=True, vmem_limit_bytes=32 * 2**20
        ),
    )(in_hbm(keys), in_hbm(values))


def shards(queries, keys, values, block_mask):
    all_keys, all_values = gathered(keys, values)
    vmem = pl.BlockSpec(memory_space=pltpu.VMEM)
    return pl.pallas_call(
        attend,
        out_shape=jax.ShapeDtypeStruct(queries.shape, jnp.float32),
        in_specs=[pl.BlockSpec(memory_space=pltpu.SMEM), vmem, vmem, vmem],
        out_specs=pl.BlockSpec(memory_space=pltpu.HBM),
        scratch_shapes=[
            pltpu.SMEM((block_mask.shape[1],), jnp.int32),
            pltpu.VMEM((DH, H * BLOCK), jnp.float32),
            pltpu.VMEM(queries.shape, jnp.float32),
            pltpu.SemaphoreType.DMA((queries.shape[0] // BLOCK,)),
        ],
        compiler_params=pltpu.CompilerParams(vmem_limit_bytes=48 * 2**20),
    )(in_hbm(block_mask), queries, all_keys, all_values)


def solution(mesh):
    placed = (P(("qrow", "kcol"), None), P(("kcol", "qrow"), None), P(("kcol", "qrow"), None), P())
    return jax.shard_map(
        shards, mesh=mesh, in_specs=placed, out_specs=P(("qrow", "kcol"), None), check_vma=False
    )
```
